256 devices in a mesh: section: 4 (over z_lo), dp: 64 (over x, z_hi, y, core).
Axes of the slice: x: 4, y: 4, z: 8 (z_hi: 2, z_lo: 4; z = z_hi * 4 + z_lo), core: 2. Of those that a mesh axis runs over, the one named last changes fastest.
Arguments:
- patches: bfloat16 [65536, 1280], P('dp'), may hold values from -16 to 16
- pre_gain: float32 [1280], replicated, may hold values from 0.1 to 1.9
- merge_gain: float32 [1280], replicated, may hold values from 0.1 to 1.9
- merge_bias: float32 [1280], replicated, may hold values from -3 to 3
- w_in: bfloat16 [1280, 2560], P('dp', 'section'), may hold values from -0.15625 to 0.15625
- w_out: bfloat16 [2560, 1280], P('section', 'dp'), may hold values from -0.125 to 0.125
- destinations: int32 [16384, 1], P(('section', 'dp')), may hold values from 0 to 63; in each aligned block of 64 rows (0 to 63, 64 to 127, ...) at most 2 rows name the same one
- upstream: bfloat16 [32768, 5120], P(('section', 'dp')), may hold values from -6 to 6
Outputs:
- received: bfloat16 [32768, 5120], P(('section', 'dp'))
- grad_w_in: float32 [1280, 2560], P('dp', 'section')
- grad_w_out: float32 [2560, 1280], P('section', 'dp')
The draws below stay inside these ranges and needn't reach their ends.
Inputs may be any that keep to these rules, and one draw needn't show every extreme that they name: `destinations`: among the 64 blocks of one device, one replica is named at most 2 times, and exactly 2 times for some replica in some devices.
All inputs are finite; a program needn't handle non-finite values.
Results may differ from the reference program's by a relative error of at most 0.0068.
Values may be sent and summed in bfloat16 or wider, within the bound.
No kernel may reach another device: no remote copies, remote signals or barrier semaphores. Data moves between devices by JAX's collectives and lax.ppermute only.
A program may use at most 128 MiB of HBM per device.

```python
import math
import jax
import jax.numpy as jnp
import numpy as np
from jax import lax

DV = 1280
FFW = 2560
MERGE = 4
BLK = 1
NBLK = 64
DM = 5120
CAP = 2
PATCH_GROUP = 1024
PATCHES = 65536
SLOTS = 128
N_SECTION = 4
N_DP = 64


def strengthened(values, own_key, source, target, parts, factor):
    owner, partner = [(jnp.arange(values.shape[dim]) // (values.shape[dim] // parts)).reshape([-1 if axis == dim else 1 for axis in range(values.ndim)]) for dim in (source, target)]
    chosen = jax.random.permutation(own_key, parts)[partner]
    strong = (owner == chosen) | (owner == (partner + parts // 2) % parts)
    return jnp.where(strong, factor * values, values)


def block_scale(key, dims, pieces, smallest, largest):
    level, own = 1.0, jax.random.fold_in(key, 6)
    for dim, shards_of in pieces:
        draws = jnp.exp(jax.random.uniform(jax.random.fold_in(own, dim), (shards_of,), jnp.float32, smallest / len(pieces), largest / len(pieces)))
        level = level * jnp.repeat(draws, dims[dim] // shards_of).reshape([-1 if axis == dim else 1 for axis in range(len(dims))])
    return level


def routed_block(key, own, number, rows, number_of, top, bound, lean):
    sequence = jax.random.permutation(key, number_of)
    packed, usual = shares(number_of, rows * top, bound, lean, True), shares(number_of, rows * top, bound, lean, False)
    places = jnp.arange(number_of)

    def named(sizes, offset_by):
        used = int((sizes > 0).sum())
        fixed = max(1, used // 4)
        moved = fixed + (places - fixed + offset_by * (used - fixed)) % max(1, number_of - fixed)
        return jnp.zeros((number_of,), jnp.int32).at[sequence[jnp.where(places < fixed, places, moved)]].set(jnp.asarray(sizes, jnp.int32))

    sizes = jnp.where(number % 4 == 0, named(packed, number // 4), named(usual, number - number // 4 - 1))
    mixed = jax.random.permutation(jax.random.fold_in(own, 3), number_of)
    giver, sink = mixed[0:number_of // 2 * 2:2], mixed[1:number_of // 2 * 2:2]
    slack = jnp.minimum(sizes[giver] - 1, bound - sizes[sink]) // 2
    slack = jnp.where((giver == sequence[0]) | (sink == sequence[0]) | (sizes[sink] == 0), 0, jnp.maximum(slack, 0))
    moved = jax.random.randint(jax.random.fold_in(own, 4), (number_of // 2,), 0, 1 << 20) % (slack + 1)
    sizes = sizes.at[giver].add(-moved).at[sink].add(moved)
    labels = jnp.searchsorted(jnp.cumsum(sizes), jnp.arange(rows * top), side="right").astype(jnp.int32)
    grid = labels.reshape(top, rows).T
    grid = grid[jax.random.permutation(jax.random.fold_in(own, 1), rows)]
    offset_by = jax.random.randint(jax.random.fold_in(own, 2), (rows, 1), 0, top)
    return jnp.take_along_axis(grid, (jnp.arange(top)[None, :] + offset_by) % top, axis=1)


def shares(number_of, total, reach, lean, full):
    loads = [(1 << 20) // math.isqrt(rank ** lean) + 1 for rank in range(1, number_of + 1)]
    largest = reach if full else min(reach, max(-(-total // number_of), total * loads[0] // sum(loads)))
    least = 1 if total - largest >= number_of - 1 else 0
    counts, spare = [largest] + [least] * (number_of - 1), total - largest - least * (number_of - 1)
    while spare > 0:
        free = [i for i in range(1, number_of) if counts[i] < largest] or [i for i in range(1, number_of) if counts[i] < reach]
        mass, left = sum([loads[i] for i in free]), spare
        for i in free:
            extra = min(reach - counts[i], max(1, left * loads[i] // mass), spare)
            counts[i] = counts[i] + extra
            spare = spare - extra
    return np.array(counts)


def noise(stream_key, shape, spread, limit, pieces=(), kind=jnp.bfloat16):
    level = block_scale(stream_key, shape, pieces, -0.22, 0.18) if pieces else 1.0
    drawn = jax.random.normal(stream_key, shape, jnp.float32) * spread * level
    return jnp.minimum(jnp.maximum(drawn, -limit), limit).astype(kind)


def heavy_noise(rng, shape, scale, reach, pieces, heavy, held_as=jnp.bfloat16):
    result = scale * jax.random.normal(rng, shape, jnp.float32)
    if pieces:
        result = result * block_scale(rng, shape, pieces, -0.22, 0.18)
    return jnp.clip(strengthened(result, jax.random.fold_in(rng, 3), *heavy), -reach, reach).astype(held_as)


def setup_inputs(seed: int = 0) -> dict:
    key_of = jax.random.split(jax.random.key(seed), 9)
    patches = heavy_noise(key_of[0], (PATCHES, DV), 1.0, 16.0, ((0, 64),), (0, 1, 64, 4.0))
    pre_gain = jnp.clip(1.0 + 0.18 * jax.random.normal(key_of[1], (DV,), jnp.float32), 0.1, 1.9)
    merge_gain = jnp.clip(1.0 + 0.18 * jax.random.normal(key_of[2], (DV,), jnp.float32), 0.1, 1.9)
    merge_bias = noise(key_of[3], (DV,), 0.5, 3.0, (), jnp.float32)
    w_in = noise(key_of[4], (DV, FFW), DV ** -0.5, 0.15625, ((0, 64), (1, 4)))
    w_out = noise(key_of[5], (FFW, DV), FFW ** -0.5, 0.125, ((0, 4), (1, 64)))
    destinations_keys = jax.random.split(jax.random.fold_in(key_of[6], 1), (N_SECTION * N_DP * NBLK) // NBLK)
    destinations_turns = jax.random.permutation(jax.random.fold_in(key_of[6], 3), (N_SECTION * N_DP * NBLK) // NBLK)
    destinations = jax.vmap(lambda own, number: routed_block(jax.random.fold_in(key_of[6], 2), own, number, NBLK, N_DP, 1, CAP, 2))(destinations_keys, destinations_turns).reshape((N_SECTION * N_DP * NBLK, 1))
    upstream = noise(key_of[7], (N_SECTION * N_DP * SLOTS, DM), 1.0, 6.0, ((0, 256),))
    return dict(patches=patches, pre_gain=pre_gain, merge_gain=merge_gain, merge_bias=merge_bias, w_in=w_in, w_out=w_out, destinations=destinations, upstream=upstream)


epsilon = 1e-06
gelu_scale = 0.7978845608028654
gelu_cubic = 0.044715

def gelu_slope(values):
    tangent = jnp.tanh(gelu_scale * (values + gelu_cubic * values * values * values))
    return 0.5 * (1.0 + tangent) + 0.5 * values * (1.0 - tangent * tangent) * gelu_scale * (1.0 + 3.0 * gelu_cubic * values * values)

def normalize(values):
    average = lax.optimization_barrier(jnp.mean(values, axis=-1, keepdims=True))
    centred = values - average
    inv_scale = lax.rsqrt(lax.optimization_barrier(jnp.mean(centred * centred, axis=-1, keepdims=True)) + epsilon)
    return (centred * inv_scale, inv_scale)

def norm_backward(cotangent, unit_rows, inv_scale, gain):
    scaled = cotangent * gain
    return inv_scale * (scaled - lax.optimization_barrier(jnp.mean(scaled, axis=-1, keepdims=True)) - unit_rows * lax.optimization_barrier(jnp.mean(scaled * unit_rows, axis=-1, keepdims=True)))

def block_ranks(targets):
    block_count = targets.shape[-1]
    matches = targets[..., :, None] == targets[..., None, :]
    earlier = lax.broadcasted_iota(jnp.int32, (block_count, block_count), 1) < lax.broadcasted_iota(jnp.int32, (block_count, block_count), 0)
    return lax.optimization_barrier(jnp.sum((matches & earlier).astype(jnp.int32), axis=-1))

def reference(patches, pre_gain, merge_gain, merge_bias, w_in, w_out, destinations, upstream):
    group_rows = PATCH_GROUP
    block_width = BLK * MERGE * DV

    def forward(replica):
        group_x = lax.dynamic_slice_in_dim(patches, (replica * group_rows).astype(jnp.int32), group_rows, 0).astype(jnp.float32)
        unit_rows, _ = normalize(group_x)
        normed = (unit_rows * pre_gain).astype(jnp.bfloat16)
        preact = jnp.dot(normed, w_in, preferred_element_type=jnp.float32)
        hidden = jax.nn.gelu(preact, approximate=True).astype(jnp.bfloat16)
        residual = group_x + jnp.dot(hidden, w_out, preferred_element_type=jnp.float32)
        unit_out, _ = normalize(residual)
        merged = (unit_out * merge_gain + merge_bias).astype(jnp.bfloat16)
        return (normed, preact, residual, merged)
    normed_all, preact_all, residual_all, merged_all = lax.map(forward, jnp.arange(N_DP, dtype=jnp.int32))
    blocks = merged_all.reshape(N_DP, N_SECTION, NBLK, block_width).transpose(1, 0, 2, 3).reshape(N_SECTION * N_DP * NBLK, block_width)
    targets = destinations.reshape(N_SECTION * N_DP, NBLK)
    block_rank = block_ranks(targets)
    device_ids = lax.broadcasted_iota(jnp.int32, (N_SECTION * N_DP, NBLK), 0)
    slot_index = ((device_ids // N_DP * N_DP + targets) * N_DP + device_ids % N_DP) * CAP + block_rank
    slot_index = slot_index.reshape(-1).astype(jnp.int32)
    received = jnp.zeros((N_SECTION * N_DP * N_DP * CAP, block_width), jnp.bfloat16).at[slot_index].set(blocks)
    received = received.reshape(N_SECTION * N_DP * N_DP * CAP * BLK, MERGE * DV)
    back_blocks = upstream.reshape(N_SECTION * N_DP * N_DP * CAP, block_width)[slot_index]
    back_rows = back_blocks.reshape(N_SECTION, N_DP, NBLK, block_width).transpose(1, 0, 2, 3).reshape(N_DP, group_rows, DV)

    def accumulate(totals, sample_item):
        normed, preact, residual, cotangent = sample_item
        unit_rows, inv_scale = normalize(residual)
        grad_residual = norm_backward(cotangent.astype(jnp.float32), unit_rows, inv_scale, merge_gain).astype(jnp.bfloat16)
        grad_hidden = lax.dot_general(grad_residual, w_out, (((1,), (1,)), ((), ())), preferred_element_type=jnp.float32)
        grad_preact = (grad_hidden * gelu_slope(preact)).astype(jnp.bfloat16)
        hidden = jax.nn.gelu(preact, approximate=True).astype(jnp.bfloat16)
        grad_first = totals[0] + lax.dot_general(normed, grad_preact, (((0,), (0,)), ((), ())), preferred_element_type=jnp.float32)
        grad_second = totals[1] + lax.dot_general(hidden, grad_residual, (((0,), (0,)), ((), ())), preferred_element_type=jnp.float32)
        return ((grad_first, grad_second), None)
    start_totals = (jnp.zeros((DV, FFW), jnp.float32), jnp.zeros((FFW, DV), jnp.float32))
    (grad_w_in, grad_w_out), _ = lax.scan(accumulate, start_totals, (normed_all, preact_all, residual_all, back_rows))
    return (received, grad_w_in, grad_w_out)
```

```python
import jax
import jax.numpy as jnp
from jax import lax
from jax.sharding import Mesh
from jax.sharding import PartitionSpec as P

DP = ("dp_0", "dp_1", "dp_2", "dp_3")
SECTION_DP = ("section",) + DP
X, Y, CORE = "dp_0", "dp_2", "dp_3"
Z = ("section", "dp_1")
XZ, YC = ("dp_0", "dp_1"), ("dp_2", "dp_3")
F32, BF16 = jnp.float32, jnp.bfloat16


epsilon = 1e-06
gelu_scale = 0.7978845608028654
gelu_cubic = 0.044715


def gelu_slope(values):
    tangent = jnp.tanh(gelu_scale * (values + gelu_cubic * values * values * values))
    return 0.5 * (1.0 + tangent) + 0.5 * values * (1.0 - tangent * tangent) * gelu_scale * (
        1.0 + 3.0 * gelu_cubic * values * values
    )


def normalize(values):
    average = jnp.mean(values, axis=-1, keepdims=True)
    centred = values - average
    inv_scale = lax.rsqrt(jnp.mean(centred * centred, axis=-1, keepdims=True) + epsilon)
    return (centred * inv_scale, inv_scale)


def norm_backward(cotangent, unit_rows, inv_scale, gain):
    scaled = cotangent * gain
    return inv_scale * (
        scaled
        - jnp.mean(scaled, axis=-1, keepdims=True)
        - unit_rows * jnp.mean(scaled * unit_rows, axis=-1, keepdims=True)
    )


def block_ranks(targets):
    block_count = targets.shape[-1]
    matches = targets[:, None] == targets[None, :]
    earlier = lax.broadcasted_iota(jnp.int32, (block_count, block_count), 1) < lax.broadcasted_iota(
        jnp.int32, (block_count, block_count), 0
    )
    return jnp.sum((matches & earlier).astype(jnp.int32), axis=-1)


def dot(a, b, dims=((1,), (0,))):
    return lax.dot_general(a, b, (dims, ((), ())), preferred_element_type=F32)


def moved(a, b, dims=((1,), (0,))):
    return dot(a, b, dims).astype(BF16)


def shift(v, axis, by):
    size = lax.axis_size(axis)
    return lax.ppermute(v, axis, [(i, (i + by) % size) for i in range(size)])


OFFSETS = (0, -1, 1, 2)


def ring_gather(v, axis):
    half = v.shape[0] // 2
    left, right = shift(v, axis, 1), shift(v, axis, -1)
    top = shift(left[:half], axis, 1)
    bottom = shift(right[half:], axis, -1)
    return [v, left, right, (top, bottom)]


def ring_reduce(own, minus, plus, across, axis):
    half = own.shape[0] // 2
    top = shift(across[:half], axis, -1)
    bottom = shift(across[half:], axis, 1)
    minus = jnp.concatenate(
        [(minus[:half].astype(F32) + top.astype(F32)).astype(BF16), minus[half:]]
    )
    plus = jnp.concatenate(
        [plus[:half], (plus[half:].astype(F32) + bottom.astype(F32)).astype(BF16)]
    )
    from_right, from_left = shift(minus, axis, -1), shift(plus, axis, 1)
    return (own.astype(F32) + from_right.astype(F32) + from_left.astype(F32)).astype(BF16)


def exchange(v, axes):
    return lax.all_to_all(v, axes, split_axis=0, concat_axis=0, tiled=True)


def small_gather(block, axis):
    rows = block.shape[0] // 2
    own, left, right, (top, bottom) = ring_gather(block, axis)
    first = jnp.concatenate([own[:rows], left[:rows], right[:rows], top])
    second = jnp.concatenate([own[rows:], left[rows:], right[rows:], bottom])
    return first, second


def gathered_weights(w_in, w_out):
    width = w_in.shape[1]
    rows = w_in.shape[0]
    shard = jnp.concatenate([w_in, w_out.T])
    column = exchange(jnp.broadcast_to(shard, (8, *shard.shape)), Z)
    halves = exchange(column.reshape(2, 4, 2 * rows, width), CORE)
    halves = halves.reshape(2, 2, 2, 2, rows, width)

    def block(parity):
        part = halves[:, parity]
        return part.transpose(2, 0, 1, 3, 4).reshape(2 * 4 * rows, width)

    a_first, a_second = small_gather(block(0), X)
    b_first, b_second = small_gather(block(1), Y)

    def whole(a, b):
        piece = 4 * rows
        own, left, right, (top, bottom) = ring_gather(a, Y)
        a_rows = [own, left, right, top, bottom]
        own, left, right, (top, bottom) = ring_gather(b, X)
        b_rows = []
        for y in range(4):
            cut = slice(y * piece, (y + 1) * piece)
            far = top if y < 2 else bottom
            far_cut = slice((y % 2) * piece, (y % 2 + 1) * piece)
            b_rows += [own[cut], left[cut], right[cut], far[far_cut]]
        return jnp.concatenate([jnp.concatenate(a_rows), jnp.concatenate(b_rows)], axis=1)

    return whole(a_first, b_first), whole(a_second, b_second)


def summed_gradients(first, second, rows, width):
    piece = 4 * rows

    def big(grad):
        a, b = grad[:, :width], grad[:, width:]
        a = ring_reduce(*[a[j * 4 * piece : (j + 1) * 4 * piece] for j in range(4)], Y)
        columns = [
            jnp.concatenate([b[(y * 4 + j) * piece : (y * 4 + j + 1) * piece] for y in range(4)])
            for j in range(4)
        ]
        return a, ring_reduce(*columns, X)

    a_second, b_second = big(second)
    a_first, b_first = big(first)

    def small(one, two, axis):
        blocks = [
            jnp.concatenate(
                [one[j * piece : (j + 1) * piece], two[j * piece : (j + 1) * piece]]
            )
            for j in range(4)
        ]
        return ring_reduce(*blocks, axis)

    a, b = small(a_first, a_second, X), small(b_first, b_second, Y)
    both = jnp.stack([a.reshape(2, 2, 2, rows, width), b.reshape(2, 2, 2, rows, width)])
    both = both.transpose(2, 0, 3, 1, 4, 5).reshape(2, 4, 2 * rows, width)
    column = exchange(both, CORE).reshape(8, 2 * rows, width)
    total = jnp.sum(exchange(column, Z).astype(F32), axis=0)
    return total[:rows], total[rows:].T


def on_device(patches, pre_gain, merge_gain, merge_bias, w_in, w_out, destinations, upstream):
    sections = lax.axis_size("section")
    share = patches.shape[0] // sections
    features = patches.shape[1]
    rows, width = w_in.shape
    block_count = destinations.shape[0]
    per_block = share // block_count
    slots = upstream.shape[0]
    capacity = slots // 64
    merged_width = upstream.shape[1]

    place = lax.broadcasted_iota(jnp.int32, (1, features), 1)
    row, rest = place % rows, place // rows
    z_hi, core, x_step, y_step = rest % 2, (rest // 2) % 2, (rest // 4) % 4, rest // 16

    def coordinate(step, axis):
        offset = jnp.where(step == 0, 0, jnp.where(step == 1, 3, step - 1))
        return (lax.axis_index(axis) + offset) % 4

    source = (((coordinate(x_step, X) * 2 + z_hi) * 4 + coordinate(y_step, Y)) * 2 + core) * rows + row
    chosen = lax.broadcasted_iota(jnp.int32, (features, features), 0) == source
    to_arrival = chosen.astype(BF16)

    first_rows = lax.dynamic_slice_in_dim(patches, lax.axis_index("section") * share, share, 0)
    new_row = lax.broadcasted_iota(jnp.int32, (share, share), 0)
    old_row = lax.broadcasted_iota(jnp.int32, (share, share), 1)
    by_row = (
        old_row == (new_row % block_count) * per_block + new_row // block_count
    ).astype(BF16)
    inputs = moved(moved(by_row, first_rows), to_arrival).astype(F32)
    gains = lax.dot_general(
        jnp.stack([pre_gain, merge_gain, merge_bias]),
        chosen.astype(F32),
        (((1,), (0,)), ((), ())),
        precision=lax.Precision.HIGHEST,
        preferred_element_type=F32,
    )
    pre_gain, merge_gain, merge_bias = gains[0], gains[1], gains[2]
    normed = (normalize(inputs)[0] * pre_gain).astype(BF16)
    normed = jnp.concatenate([normed, shift(normed, CORE, 1)])

    targets = destinations[:, 0]
    slot = ((targets % 8) * 8 + targets // 8) * capacity + block_ranks(targets)
    picker = (
        slot[:, None] == lax.broadcasted_iota(jnp.int32, (block_count, slots), 1)
    ).astype(BF16)
    a = lax.broadcasted_iota(jnp.int32, (slots, slots), 0)
    b = lax.broadcasted_iota(jnp.int32, (slots, slots), 1)
    swapped = (((a // capacity % 8) * 8 + a // capacity // 8) * capacity + a % capacity) == b
    swapped = swapped.astype(BF16)

    first, second = gathered_weights(w_in, w_out)

    coming = exchange(upstream.reshape(8, slots // 8, merged_width), XZ)
    coming = moved(swapped, coming.reshape(slots, merged_width))
    coming = exchange(coming.reshape(8, slots // 8, merged_width), YC)
    cotangent = moved(picker, coming.reshape(slots, merged_width))
    cotangent = jnp.concatenate(
        [cotangent[:, q * features : (q + 1) * features] for q in range(per_block)]
    )
    cotangent = moved(cotangent, to_arrival)

    preact = dot(normed, first)
    hidden = jax.nn.gelu(preact, approximate=True).astype(BF16)
    partial = dot(hidden, second, ((1,), (1,)))
    residual = inputs + partial[:share] + shift(partial[share:].astype(BF16), CORE, 1).astype(F32)
    unit_out, scale_out = normalize(residual)
    merged = (unit_out * merge_gain + merge_bias).astype(BF16)
    grad_own = norm_backward(cotangent.astype(F32), unit_out, scale_out, merge_gain).astype(BF16)
    grad_residual = jnp.concatenate([grad_own, shift(grad_own, CORE, 1)])

    merged = moved(merged, to_arrival, ((1,), (1,)))
    blocks = jnp.concatenate(
        [merged[q * block_count : (q + 1) * block_count] for q in range(per_block)], axis=1
    )
    outgoing = moved(picker, blocks, ((0,), (0,)))
    outgoing = exchange(outgoing.reshape(8, slots // 8, merged_width), YC)
    outgoing = moved(swapped, outgoing.reshape(slots, merged_width))
    received = exchange(outgoing.reshape(8, slots // 8, merged_width), XZ)
    received = received.reshape(slots, merged_width)

    grad_second = moved(grad_residual, hidden, ((0,), (0,)))
    grad_hidden = dot(grad_residual, second)
    grad_preact = (grad_hidden * gelu_slope(preact)).astype(BF16)
    grad_first = moved(normed, grad_preact, ((0,), (0,)))
    grad_w_in, grad_w_out = summed_gradients(grad_first, grad_second, rows, width)
    return (received, grad_w_in, grad_w_out)


def solution(mesh):
    finer = Mesh(mesh.devices.reshape(mesh.shape["section"], 4, 2, 4, 2), SECTION_DP)
    in_specs = (
        P(DP, None),
        P(),
        P(),
        P(),
        P(DP, "section"),
        P("section", DP),
        P(SECTION_DP, None),
        P(SECTION_DP, None),
    )
    out_specs = (P(SECTION_DP, None), P(DP, "section"), P("section", DP))
    return jax.shard_map(
        on_device, mesh=finer, in_specs=in_specs, out_specs=out_specs, check_vma=False
    )
```
